32 devices in a mesh: head: 4 (over y, core), row: 8 (over z, x).
Axes of the slice: x: 2, y: 2, z: 4, core: 2. Of those that a mesh axis runs over, the one named last changes fastest.
Arguments:
- hidden_in: bfloat16 [512, 2048], replicated, may hold values from -6 to 6
- w_query: bfloat16 [2048, 16, 128], P(None, 'head', 'row'), may hold values from -0.125 to 0.125
- w_key: bfloat16 [2048, 16, 128], P(None, 'head', 'row'), may hold values from -0.125 to 0.125
- w_value: bfloat16 [2048, 32, 128], P(None, 'head'), may hold values from -0.125 to 0.125
- w_zgate: bfloat16 [2048, 32, 128], P(None, 'head'), may hold values from -0.125 to 0.125
- w_decay: bfloat16 [2048, 32], P(None, 'head'), may hold values from -0.125 to 0.125
- w_beta: bfloat16 [2048, 32], P(None, 'head'), may hold values from -0.125 to 0.125
- decay_log: float32 [32], P('head'), may hold values from -1.5 to 1.5
- dt_bias: float32 [32], P('head'), may hold values from -2 to 2
- norm_gain: float32 [128], replicated, may hold values from 0.1 to 1.9
- w_out: bfloat16 [32, 128, 2048], P('head'), may hold values from -0.09375 to 0.09375
- state: float32 [512, 32, 128, 128], P(None, 'head', 'row'), may hold values from -6 to 6
Outputs:
- layer_out: bfloat16 [512, 2048], P('row', 'head')
- new_state: float32 [512, 32, 128, 128], P(None, 'head', 'row')
The draws below stay inside these ranges and needn't reach their ends.
All inputs are finite; a program needn't handle non-finite values.
Results may differ from the reference program's by a relative error of at most 0.005.
Values sent between devices are 32-bit elements; how exact they have to be, the bound alone decides.
A program may use at most 128 MiB of HBM per device.

```python
import jax
import jax.numpy as jnp
from jax import lax

D = 2048
H = 32
HK = 16
K = 128
V = 128
SEQS = 512


def block_levels(rng, extent, shards, least, top_value):
    loudness = 1.0
    for dim, parts in shards:
        draws = jax.random.uniform(jax.random.fold_in(jax.random.fold_in(rng, 6), dim), (parts,), jnp.float32, least / len(shards), top_value / len(shards))
        loudness = loudness * jnp.repeat(jnp.exp(draws), extent[dim] // parts).reshape((-1,) + (1,) * (len(extent) - 1 - dim))
    return loudness


def noise(key, extent, width, reach, split=(), held_as=jnp.bfloat16):
    result = width * jax.random.normal(key, extent, jnp.float32)
    if split:
        result = result * block_levels(key, extent, split, -0.22, 0.18)
    return jnp.clip(result, -reach, reach).astype(held_as)


def setup_inputs(seed: int = 0) -> dict:
    arg_keys = jax.random.split(jax.random.key(seed), 13)
    hidden_in = noise(arg_keys[0], (SEQS, D), 1.0, 6.0)
    w_query = noise(arg_keys[1], (D, HK, K), D ** -0.5, 0.125, ((1, 4), (2, 8)))
    w_key = noise(arg_keys[2], (D, HK, K), D ** -0.5, 0.125, ((1, 4), (2, 8)))
    w_value = noise(arg_keys[3], (D, H, V), D ** -0.5, 0.125, ((1, 4),))
    w_zgate = noise(arg_keys[4], (D, H, V), D ** -0.5, 0.125, ((1, 4),))
    w_decay = noise(arg_keys[5], (D, H), D ** -0.5, 0.125, ((1, 4),))
    w_beta = noise(arg_keys[6], (D, H), D ** -0.5, 0.125, ((1, 4),))
    decay_log = jnp.clip(jax.random.uniform(arg_keys[7], (H,), jnp.float32, -1.5, 1.5) * block_levels(arg_keys[7], (H,), ((0, 4),), -0.4, 0.0), -1.5, 1.5)
    dt_bias = jnp.clip(jax.random.uniform(arg_keys[8], (H,), jnp.float32, -2.0, 2.0) * block_levels(arg_keys[8], (H,), ((0, 4),), -0.4, 0.0), -2.0, 2.0)
    norm_gain = jnp.clip(1.0 + 0.18 * jax.random.normal(arg_keys[9], (V,), jnp.float32), 0.1, 1.9)
    w_out = noise(arg_keys[10], (H, V, D), (H * V) ** -0.5, 0.09375, ((0, 4),))
    state = noise(arg_keys[11], (SEQS, H, K, V), 1.0, 6.0, ((1, 4), (2, 8)), jnp.float32)
    return {"hidden_in": hidden_in, "w_query": w_query, "w_key": w_key, "w_value": w_value, "w_zgate": w_zgate, "w_decay": w_decay, "w_beta": w_beta, "decay_log": decay_log, "dt_bias": dt_bias, "norm_gain": norm_gain, "w_out": w_out, "state": state}


def reference(hidden_in, w_query, w_key, w_value, w_zgate, w_decay, w_beta, decay_log, dt_bias, norm_gain, w_out, state):
    xf = hidden_in.astype(jnp.float32)
    query = jnp.einsum('bd,dhk->bhk', xf, w_query.astype(jnp.float32))
    keys = jnp.einsum('bd,dhk->bhk', xf, w_key.astype(jnp.float32))
    values = jnp.einsum('bd,dhv->bhv', xf, w_value.astype(jnp.float32))
    zgate = jnp.einsum('bd,dhv->bhv', xf, w_zgate.astype(jnp.float32))
    decay_in = jnp.dot(hidden_in, w_decay, preferred_element_type=jnp.float32) + dt_bias
    decay = jnp.exp(-jnp.exp(decay_log) * jax.nn.softplus(decay_in))
    beta = jax.nn.sigmoid(jnp.dot(hidden_in, w_beta, preferred_element_type=jnp.float32))
    group = state.shape[1] // keys.shape[1]
    query_unit = query * lax.rsqrt(1.0 + lax.optimization_barrier(jnp.sum(query * query, axis=-1, keepdims=True)))
    key_unit = keys * lax.rsqrt(1.0 + lax.optimization_barrier(jnp.sum(keys * keys, axis=-1, keepdims=True)))
    query_wide = jnp.repeat(query_unit, group, axis=1)
    key_wide = jnp.repeat(key_unit, group, axis=1)
    readk = jnp.einsum('bhkv,bhk->bhv', state, key_wide, precision=lax.Precision.HIGHEST)
    delta = beta[..., None] * (values - decay[..., None] * readk)
    new_state = decay[..., None, None] * state + key_wide[..., None] * delta[:, :, None, :]
    readq = jnp.einsum('bhkv,bhk->bhv', new_state, query_wide, precision=lax.Precision.HIGHEST)
    meansq = lax.optimization_barrier(jnp.mean(readq * readq, axis=-1, keepdims=True))
    normed = (readq * lax.rsqrt(meansq + 0.5) * norm_gain * jax.nn.silu(zgate)).astype(jnp.bfloat16)
    layer_out = jnp.einsum('bhv,hvd->bd', normed.astype(jnp.float32), w_out.astype(jnp.float32))
    return (layer_out.astype(jnp.bfloat16), new_state)
```

```python
import functools

import jax
import jax.numpy as jnp
from jax import lax
from jax.experimental import pallas as pl
from jax.experimental.pallas import tpu as pltpu
from jax.sharding import PartitionSpec as P

MESH = pl.DeviceIdType.MESH
F32 = jnp.float32
BF16 = jnp.bfloat16


def head_mask(heads, depth, group_rows):
    lane = lax.broadcasted_iota(jnp.int32, (group_rows, heads * depth), 1)
    row = lax.broadcasted_iota(jnp.int32, (group_rows, heads * depth), 0)
    low = row * depth
    return (lane >= low) & (lane < low + depth)


def read_kernel(heads, depth, q_ref, k_ref, s_ref, rk_ref, rq_ref):
    seqs, _, width = s_ref.shape
    mask = head_mask(heads, depth, heads)

    def body(b, carry):
        krow = jnp.broadcast_to(k_ref[pl.ds(b, 1), :], (heads, heads * depth))
        qrow = jnp.broadcast_to(q_ref[pl.ds(b, 1), :], (heads, heads * depth))
        left = jnp.concatenate([jnp.where(mask, krow, 0.0), jnp.where(mask, qrow, 0.0)], axis=0)
        read = jnp.dot(
            left.astype(BF16), s_ref[b].astype(BF16), preferred_element_type=F32
        )
        at = pl.multiple_of(b * heads, heads)
        rk_ref[pl.ds(at, heads), :] = read[:heads]
        rq_ref[pl.ds(at, heads), :] = read[heads:]
        return carry

    lax.fori_loop(0, seqs, body, 0, unroll=8)


def update_kernel(heads, depth, k_ref, decay_ref, delta_ref, s_ref, out_ref):
    seqs, _, width = s_ref.shape
    mask = head_mask(heads, depth, heads)

    def body(b, carry):
        krow = jnp.broadcast_to(k_ref[pl.ds(b, 1), :], (heads, heads * depth))
        left = jnp.where(mask, krow, 0.0).astype(BF16)
        at = pl.multiple_of(b * heads, heads)
        delta = delta_ref[pl.ds(at, heads), :].astype(BF16)
        decay = decay_ref[pl.ds(at, heads), :]
        add = lax.dot_general(
            left, delta, (((0,), (0,)), ((), ())), preferred_element_type=F32
        )
        for h in range(heads):
            rows = slice(h * depth, (h + 1) * depth)
            out_ref[b, rows, :] = decay[h : h + 1, :] * s_ref[b, rows, :] + add[rows, :]
        return carry

    lax.fori_loop(0, seqs, body, 0, unroll=8)


def exchange_kernel(
    nx, nz, nh, heads, group, own,
    rk_ref, rq_ref, stats_ref, values_ref, zgate_ref, decay_ref, beta_ref, gain_ref, wout_ref,
    delta_ref, layer_ref,
    kx, ksum, kz, ktot, qz, qsum, qx, qtot, st, normed, part, hrecv,
    kx_s, kx_r, kz_s, kz_r, qz_s, qz_r, qx_s, qx_r, st_s, st_r,
    ax_s, ax_r, az_s, az_r, bz_s, bz_r, bx_s, bx_r, h_s, h_r,
):
    me = lax.axis_index("row")
    my_head = lax.axis_index("head")
    x = lax.rem(me, nx)
    z = lax.div(me, nx)
    nrow = nx * nz
    blk = own * heads
    half = blk // 2

    def at(index, size):
        return pl.ds(pl.multiple_of(index * size, size), size)

    barrier = pltpu.get_barrier_semaphore()
    for d in range(1, nrow):
        pl.semaphore_signal(
            barrier, inc=1, device_id={"row": lax.rem(me + d, nrow)}, device_id_type=MESH
        )
    for d in range(1, nh):
        pl.semaphore_signal(
            barrier, inc=1, device_id={"head": lax.rem(my_head + d, nh)}, device_id_type=MESH
        )
    pl.semaphore_wait(barrier, nrow - 1 + nh - 1)

    def send(src, dst, ssem, rsem, row):
        copy = pltpu.make_async_remote_copy(
            src_ref=src, dst_ref=dst, send_sem=ssem, recv_sem=rsem,
            device_id={"row": row}, device_id_type=MESH,
        )
        copy.start()
        return copy

    zorder = sorted(range(nz), key=lambda d: -min(d, nz - d))
    sent = []

    stats_in = []
    for d in range(1, nrow):
        to = lax.rem(me + d, nrow)
        stats_in.append(
            send(stats_ref.at[at(to, own)], st.at[d - 1], st_s.at[d - 1], st_r.at[d - 1], to)
        )
    kx_in = {}
    for d in zorder:
        zt = lax.rem(z + d, nz)
        for e in range(1, nx):
            xt = lax.rem(x + e, nx)
            i = (e - 1) * nz + d
            kx_in[e, d] = send(
                rk_ref.at[at(zt * nx + xt, blk)], kx.at[i], kx_s.at[i], kx_r.at[i], z * nx + xt
            )
    qz_in = {}
    for d in zorder:
        if d:
            zt = lax.rem(z + d, nz)
            qz_in[d] = send(
                rq_ref.at[at(zt, nx * blk)], qz.at[d - 1], qz_s.at[d - 1], qz_r.at[d - 1],
                zt * nx + x,
            )
    kz_in = {}
    for d in zorder:
        zt = lax.rem(z + d, nz)
        total = rk_ref[at(zt * nx + x, blk), :]
        for e in range(1, nx):
            kx_in[e, d].wait_recv()
            total = total + kx[(e - 1) * nz + d]
        if d:
            ksum[d - 1] = total
            kz_in[d] = send(
                ksum.at[d - 1], kz.at[d - 1], kz_s.at[d - 1], kz_r.at[d - 1], zt * nx + x
            )
        else:
            ktot[...] = total
    stats = stats_ref[at(me, own), :]
    for d in range(1, nrow):
        stats_in[d - 1].wait_recv()
        stats = stats + st[d - 1]
    total = ktot[...]
    for d in range(1, nz):
        kz_in[d].wait_recv()
        total = total + kz[d - 1]
    ktot[...] = total

    mine = me * blk
    for h in range(heads):
        c = h // group
        kscale = lax.rsqrt(1.0 + stats[:, c : c + 1])
        cols = slice(h * 128, (h + 1) * 128)
        readk = ktot[pl.ds(h, own, stride=heads), :] * kscale
        delta = beta_ref[:, h : h + 1] * (values_ref[:, cols] - decay_ref[:, h : h + 1] * readk)
        ktot[pl.ds(h, own, stride=heads), :] = delta * kscale
    delta_ref[at(me, blk), :] = ktot[...]

    def lo(row):
        return pl.ds(pl.multiple_of(row * blk, half), half)

    def hi(row):
        return pl.ds(pl.multiple_of(row * blk + half, half), half)

    ax_in, az_in, bz_in, bx_in = {}, {}, {}, {}
    for e in range(1, nx):
        xt = lax.rem(x + e, nx)
        ax_in[e] = send(
            ktot.at[pl.ds(0, half)], delta_ref.at[lo(me)], ax_s.at[e - 1], ax_r.at[e - 1],
            z * nx + xt,
        )
    for d in zorder:
        if d:
            zt = lax.rem(z + d, nz)
            bz_in[d] = send(
                ktot.at[pl.ds(half, half)], delta_ref.at[hi(me)], bz_s.at[d - 1], bz_r.at[d - 1],
                zt * nx + x,
            )
    for d in zorder:
        if d:
            i = d - 1
            zt = lax.rem(z + d, nz)
            az_in[0, d] = send(
                ktot.at[pl.ds(0, half)], delta_ref.at[lo(me)], az_s.at[i], az_r.at[i], zt * nx + x
            )
    for e in range(1, nx):
        i = (e - 1) * nz
        xt = lax.rem(x + e, nx)
        bx_in[e, 0] = send(
            ktot.at[pl.ds(half, half)], delta_ref.at[hi(me)], bx_s.at[i], bx_r.at[i], z * nx + xt
        )
    for d in zorder:
        if d:
            qz_in[d].wait_recv()
    qx_in = {}
    for e in list(range(1, nx)) + [0]:
        xt = lax.rem(x + e, nx)
        total = rq_ref[at(z * nx + xt, blk), :]
        for d in range(1, nz):
            total = total + qz[d - 1, at(xt, blk), :]
        if e:
            qsum[e - 1] = total
            qx_in[e] = send(
                qsum.at[e - 1], qx.at[e - 1], qx_s.at[e - 1], qx_r.at[e - 1], z * nx + xt
            )
        else:
            qtot[...] = total
    for e in range(1, nx):
        ax_in[e].wait_recv()
        source = z * nx + lax.rem(x - e + nx, nx)
        for d in zorder:
            if d:
                i = e * (nz - 1) + d - 1
                zt = lax.rem(z + d, nz)
                az_in[e, d] = send(
                    delta_ref.at[lo(source)], delta_ref.at[lo(source)], az_s.at[i], az_r.at[i],
                    zt * nx + x,
                )
    for d in sorted(range(1, nz), key=lambda d: min(d, nz - d)):
        bz_in[d].wait_recv()
        source = lax.rem(z - d + nz, nz) * nx + x
        for e in range(1, nx):
            i = (e - 1) * nz + d
            xt = lax.rem(x + e, nx)
            bx_in[e, d] = send(
                delta_ref.at[hi(source)], delta_ref.at[hi(source)], bx_s.at[i], bx_r.at[i],
                z * nx + xt,
            )
    total = qtot[...]
    for e in range(1, nx):
        qx_in[e].wait_recv()
        total = total + qx[e - 1]
    qtot[...] = total
    hk = heads // group
    for h in range(heads):
        c = h // group
        kscale = lax.rsqrt(1.0 + stats[:, c : c + 1])
        qscale = lax.rsqrt(1.0 + stats[:, hk + c : hk + c + 1])
        unit = stats[:, 2 * hk + c : 2 * hk + c + 1] * qscale
        cols = slice(h * 128, (h + 1) * 128)
        readq = (
            decay_ref[:, h : h + 1] * (qtot[pl.ds(h, own, stride=heads), :] * qscale)
            + unit * ktot[pl.ds(h, own, stride=heads), :]
        )
        meansq = jnp.mean(readq * readq, axis=-1, keepdims=True)
        gate = jax.nn.silu(zgate_ref[:, cols])
        out = readq * lax.rsqrt(meansq + 0.5) * gain_ref[...] * gate
        normed[:, cols] = out.astype(BF16)
    width = layer_ref.shape[1]
    h_in = {}
    for d in list(range(1, nh)) + [0]:
        to = lax.rem(my_head + d, nh)
        part[d] = jnp.dot(
            normed[...], wout_ref[:, at(to, width)], preferred_element_type=F32
        )
        if d:
            h_in[d] = pltpu.make_async_remote_copy(
                src_ref=part.at[d], dst_ref=hrecv.at[d - 1], send_sem=h_s.at[d - 1],
                recv_sem=h_r.at[d - 1], device_id={"head": to}, device_id_type=MESH,
            )
            h_in[d].start()
    total = part[0]
    for d in range(1, nh):
        h_in[d].wait_recv()
        total = total + hrecv[d - 1]
    layer_ref[...] = total.astype(BF16)

    for group_in in (az_in, bx_in):
        for key, copy in group_in.items():
            copy.wait_recv()
    for group_in in (kx_in, qz_in, kz_in, ax_in, az_in, bz_in, bx_in, qx_in, h_in):
        for key, copy in group_in.items():
            copy.wait_send()
    for copy in stats_in:
        copy.wait_send()


def split_rows(rows):
    nx = 1
    while (2 * nx) * (2 * nx) <= rows:
        nx *= 2
    return nx, rows // nx


def local(
    hidden_in, w_query, w_key, w_value, w_zgate, w_decay, w_beta, decay_log, dt_bias,
    norm_gain, w_out, state,
):
    seqs, model = hidden_in.shape
    _, hk, depth = w_key.shape
    heads, width = state.shape[1], state.shape[3]
    group = heads // hk
    wide = heads * depth
    nrow, nh = lax.axis_size("row"), lax.axis_size("head")
    nx, nz = split_rows(nrow)
    own = seqs // nrow
    first = lax.axis_index("row") * own

    w_qk = jnp.concatenate(
        [
            jnp.repeat(w_query, group, axis=1).reshape(model, wide),
            jnp.repeat(w_key, group, axis=1).reshape(model, wide),
        ],
        axis=1,
    )
    qk = jnp.dot(hidden_in, w_qk, preferred_element_type=F32)
    query, keys = qk[:, :wide], qk[:, wide:]
    cols = jnp.arange(wide)
    pick = ((cols[:, None] // (depth * group)) == jnp.arange(hk)[None, :]) & (
        (cols[:, None] // depth) % group == 0
    )

    def head_sum(array):
        return jnp.dot(array, pick.astype(F32), precision=lax.Precision.HIGHEST)

    stats = jnp.concatenate(
        [head_sum(keys * keys), head_sum(query * query), head_sum(query * keys)], axis=1
    )
    stats = jnp.pad(stats, ((0, 0), (0, 128 - 3 * hk)))
    small = jnp.dot(
        hidden_in, jnp.concatenate([w_decay, w_beta], axis=1), preferred_element_type=F32
    )
    decay = jnp.exp(-jnp.exp(decay_log) * jax.nn.softplus(small[:, :heads] + dt_bias))
    beta = jax.nn.sigmoid(small[:, heads:])
    decay_wide = jnp.broadcast_to(decay[:, :, None], (seqs, heads, width)).reshape(-1, width)
    own_hidden = lax.dynamic_slice_in_dim(hidden_in, first, own, 0)
    own_decay = lax.dynamic_slice_in_dim(decay, first, own, 0)
    own_beta = lax.dynamic_slice_in_dim(beta, first, own, 0)
    values = jnp.einsum("bd,dhv->bhv", own_hidden, w_value, preferred_element_type=F32)
    zgate = jnp.einsum("bd,dhv->bhv", own_hidden, w_zgate, preferred_element_type=F32)

    flat = state.reshape(seqs, wide, width)
    step = 32
    row_spec = pl.BlockSpec((step, wide), lambda i: (i, 0))
    head_spec = pl.BlockSpec((step * heads, width), lambda i: (i, 0))
    state_spec = pl.BlockSpec((step, wide, width), lambda i: (i, 0, 0))
    by_head = jax.ShapeDtypeStruct((seqs * heads, width), F32)
    rk, rq = pl.pallas_call(
        functools.partial(read_kernel, heads, depth),
        grid=(seqs // step,),
        in_specs=[row_spec, row_spec, state_spec],
        out_specs=[head_spec, head_spec],
        out_shape=[by_head, by_head],
        name="read",
    )(query, keys, flat)

    blk = own * heads
    vmem = pl.BlockSpec(memory_space=pltpu.VMEM)
    dma = lambda n: pltpu.SemaphoreType.DMA((n,))
    delta, layer_out = pl.pallas_call(
        functools.partial(exchange_kernel, nx, nz, nh, heads, group, own),
        in_specs=[vmem] * 9,
        out_specs=[vmem] * 2,
        out_shape=[by_head, jax.ShapeDtypeStruct((own, w_out.shape[2] // nh), BF16)],
        scratch_shapes=[
            pltpu.VMEM(((nx - 1) * nz, blk, width), F32),
            pltpu.VMEM((nz - 1, blk, width), F32),
            pltpu.VMEM((nz - 1, blk, width), F32),
            pltpu.VMEM((blk, width), F32),
            pltpu.VMEM((nz - 1, nx * blk, width), F32),
            pltpu.VMEM((nx - 1, blk, width), F32),
            pltpu.VMEM((nx - 1, blk, width), F32),
            pltpu.VMEM((blk, width), F32),
            pltpu.VMEM((nrow - 1, own, 128), F32),
            pltpu.VMEM((own, heads * width), BF16),
            pltpu.VMEM((nh, own, w_out.shape[2] // nh), F32),
            pltpu.VMEM((nh - 1, own, w_out.shape[2] // nh), F32),
            dma((nx - 1) * nz), dma((nx - 1) * nz), dma(nz - 1), dma(nz - 1),
            dma(nz - 1), dma(nz - 1), dma(nx - 1), dma(nx - 1), dma(nrow - 1), dma(nrow - 1),
            dma(nx - 1), dma(nx - 1), dma(nx * (nz - 1)), dma(nx * (nz - 1)),
            dma(nz - 1), dma(nz - 1), dma((nx - 1) * nz), dma((nx - 1) * nz),
            dma(nh - 1), dma(nh - 1),
        ],
        compiler_params=pltpu.CompilerParams(
            collective_id=0, has_side_effects=True, vmem_limit_bytes=48 * 1024 * 1024
        ),
        name="exchange",
    )(
        rk, rq, stats, values.reshape(own, -1), zgate.reshape(own, -1), own_decay, own_beta,
        norm_gain.reshape(1, -1), w_out.reshape(-1, w_out.shape[2]),
    )

    new_state = pl.pallas_call(
        functools.partial(update_kernel, heads, depth),
        grid=(seqs // step,),
        in_specs=[row_spec, head_spec, head_spec, state_spec],
        out_specs=state_spec,
        out_shape=jax.ShapeDtypeStruct(flat.shape, F32),
        name="update",
    )(keys, decay_wide, delta, flat)
    return (layer_out, new_state.reshape(state.shape))


def solution(mesh):
    in_specs = (
        P(),
        P(None, "head", "row"),
        P(None, "head", "row"),
        P(None, "head", None),
        P(None, "head", None),
        P(None, "head"),
        P(None, "head"),
        P("head"),
        P("head"),
        P(),
        P("head", None, None),
        P(None, "head", "row", None),
    )
    out_specs = (P("row", "head"), P(None, "head", "row", None))
    return jax.shard_map(local, mesh=mesh, in_specs=in_specs, out_specs=out_specs, check_vma=False)
```
